32 devices in a mesh: dp: 8 (over z, x), param: 4 (over y, core).
Axes of the slice: x: 2, y: 2, z: 4, core: 2. Of those that a mesh axis runs over, the one named last changes fastest.
Arguments:
- ex_grads: bfloat16 [768, 5120], P('dp', 'param'), may hold values from -6 to 6
- tgt_grads: bfloat16 [2048, 5120], P('dp', 'param'), may hold values from -6 to 6
- projection: bfloat16 [5120, 4096], P('param'), may hold values from -0.078125 to 0.078125
- example_weight: float32 [768], P('param'), may hold values from 0.05 to 1
Outputs:
- scores: float32 [2048, 768], P('dp', 'param')
The draws below stay inside these ranges and needn't reach their ends.
All inputs are finite; a program needn't handle non-finite values.
Results may differ from the reference program's by a relative error of at most 0.0078.
Values may be sent and summed in bfloat16 or wider, within the bound.
A program may use at most 192 MiB of HBM per device.

```python
import math
import jax
import jax.numpy as jnp

COLS = 4096
EXAMPLES = 768
TARGETS = 2048
PARAMS = 5120


def latent_setup(key):
    count = min(48, COLS // 2, PARAMS // 2, EXAMPLES // 4)
    top_value = EXAMPLES / 4.0
    low_value = 3.0
    fraction = jnp.arange(count, dtype=jnp.float32) / (count - 1)
    eigen = top_value * jnp.power(jnp.float32(low_value / top_value), fraction)
    scales = jnp.sqrt(eigen / EXAMPLES)
    basis = jax.random.normal(jax.random.fold_in(key, 101), (count, PARAMS), jnp.float32)
    common = jax.random.normal(jax.random.fold_in(key, 103), (PARAMS,), jnp.float32)
    return (scales, basis, common)


def spread_values(key, dims):
    return jax.random.normal(key, dims, jnp.float32)


def draw_ex_grads(key, part):
    scales, basis, common = latent_setup(key)
    count = scales.shape[0]
    coeff = spread_values(jax.random.fold_in(key, 201), (EXAMPLES, count))
    noise = spread_values(jax.random.fold_in(key, 202), (EXAMPLES, PARAMS))
    loading = jax.random.uniform(jax.random.fold_in(key, 203), (EXAMPLES, 1), jnp.float32, minval=0.5, maxval=1.5)
    common_scale = 0.7
    values = jnp.dot(coeff * scales[None, :], basis) + common_scale * loading * common[None, :] + noise
    return jnp.clip(values, -6.0, 6.0).astype(jnp.bfloat16)


def draw_tgt_grads(key, part):
    scales, basis, common = latent_setup(key)
    count = scales.shape[0]
    coeff = spread_values(jax.random.fold_in(key, 301), (TARGETS, count))
    noise = spread_values(jax.random.fold_in(key, 302), (TARGETS, PARAMS))
    values = jnp.dot(coeff * scales[None, :], basis) + noise
    return jnp.clip(values, -6.0, 6.0).astype(jnp.bfloat16)


def levels(rng, shape, pieces, low, high):
    gain = 1.0
    for dim, shards_of in pieces:
        steps = jax.random.uniform(jax.random.fold_in(jax.random.fold_in(rng, 6), dim), (shards_of,), jnp.float32, low / len(pieces), high / len(pieces))
        gain = gain * jnp.repeat(jnp.exp(steps), shape[dim] // shards_of).reshape((-1,) + (1,) * (len(shape) - 1 - dim))
    return gain


def scatter_about(own_key, shape, width, reach, split=(), kind=jnp.bfloat16):
    values = width * jax.random.normal(own_key, shape, jnp.float32)
    if split:
        values = values * levels(own_key, shape, split, -0.22, 0.18)
    return jnp.clip(values, -reach, reach).astype(kind)


def setup_inputs(seed: int = 0) -> dict:
    arg_keys = jax.random.split(jax.random.key(seed), 5)
    ex_grads = draw_ex_grads(jax.random.fold_in(arg_keys[4], 71), 0)
    tgt_grads = draw_tgt_grads(jax.random.fold_in(arg_keys[4], 71), 0)
    projection = scatter_about(arg_keys[2], (PARAMS, COLS), PARAMS ** -0.5, 0.078125, ((0, 4),))
    example_weight = jnp.clip(jnp.exp(math.log(1.0) - 2.9957323 * jax.random.uniform(arg_keys[3], (EXAMPLES,), jnp.float32) ** levels(arg_keys[3], (EXAMPLES,), ((0, 4),), -0.2, 0.2)), 0.05, 1.0)
    return dict(ex_grads=ex_grads, tgt_grads=tgt_grads, projection=projection, example_weight=example_weight)


ridge_value = 0.5

def reference(ex_grads, tgt_grads, projection, example_weight):
    train_feat = jnp.dot(ex_grads.astype(jnp.float32), projection.astype(jnp.float32), preferred_element_type=jnp.float32).astype(jnp.bfloat16)
    target_feat = jnp.dot(tgt_grads.astype(jnp.float32), projection.astype(jnp.float32), preferred_element_type=jnp.float32).astype(jnp.bfloat16)
    examples = train_feat.shape[0]
    kernel = jnp.dot(train_feat.astype(jnp.float32), train_feat.T.astype(jnp.float32), preferred_element_type=jnp.float32) / COLS
    kernel = kernel + ridge_value * jnp.eye(examples, dtype=jnp.float32)
    cross = jnp.dot(target_feat.astype(jnp.float32), train_feat.T.astype(jnp.float32), preferred_element_type=jnp.float32) / COLS
    factor = jnp.linalg.cholesky(kernel)
    forward = jax.scipy.linalg.solve_triangular(factor, cross.T, lower=True)
    solved = jax.scipy.linalg.solve_triangular(factor, forward, lower=True, trans=1)
    return solved.T * math.sqrt(COLS) * example_weight[None, :]
```

```python
import functools
import math

import jax
import jax.numpy as jnp
from jax import lax
from jax.experimental import pallas as pl
from jax.experimental.pallas import tpu as pltpu
from jax.sharding import PartitionSpec as P

ridge_value = 0.5
LANES = 128
GROUP = 8


def dot32(a, b):
    return jnp.dot(a, b, preferred_element_type=jnp.float32, precision=lax.Precision.HIGHEST)


def invert_block(block):
    size = block.shape[0]
    groups = size // GROUP
    rows = [block[GROUP * i : GROUP * (i + 1), :] for i in range(groups)]
    shape = (GROUP, size)
    sub = lax.broadcasted_iota(jnp.int32, shape, 0)
    lane = lax.broadcasted_iota(jnp.int32, shape, 1)

    def lane_splat(x, c):
        return jnp.broadcast_to(x[:, c : c + 1], shape)

    def row_splat(x, j):
        return jnp.broadcast_to(x[j : j + 1, :], shape)

    for g in range(groups):
        base = GROUP * g
        panel = rows[g]
        cols = [lane_splat(panel, base + j) for j in range(GROUP)]
        in_group = (lane >= base) & (lane < base + GROUP)
        panel = jnp.where(in_group, jnp.where(sub + base == lane, 1.0, 0.0), panel)
        for j in range(GROUP):
            inv = 1.0 / row_splat(cols[j], j)
            mult = jnp.where(sub == j, 1.0 - inv, cols[j] * inv)
            for c in range(j + 1, GROUP):
                cols[c] = cols[c] - mult * row_splat(cols[c], j)
            panel = panel - mult * row_splat(panel, j)
        spread = [row_splat(panel, j) for j in range(GROUP)]
        order = list(range(g + 1, groups)) + list(range(g))
        for i in order:
            acc = jnp.where(in_group, 0.0, rows[i])
            for j in range(GROUP):
                acc = acc - lane_splat(rows[i], base + j) * spread[j]
            rows[i] = acc
        rows[g] = panel
    return jnp.concatenate(rows, axis=0)


def solve_kernel(columns, kernel_ref, cross_ref, weight_ref, out_ref, a_ref, b_ref, inv_ref):
    n = kernel_ref.shape[0]
    blocks = n // LANES
    diag = lax.broadcasted_iota(jnp.int32, (LANES, n), 0)
    col_ids = lax.broadcasted_iota(jnp.int32, (LANES, n), 1)
    for i in range(blocks):
        part = kernel_ref[i * LANES : (i + 1) * LANES, :] / columns
        a_ref[i * LANES : (i + 1) * LANES, :] = part + jnp.where(diag + i * LANES == col_ids, ridge_value, 0.0)
    b_ref[...] = cross_ref[...] / columns

    def step(k, carry):
        at = pl.multiple_of(k * LANES, LANES)
        inv_ref[...] = invert_block(a_ref[pl.ds(at, LANES), pl.ds(at, LANES)])
        for kk in range(blocks):

            @pl.when(k == kk)
            def _():
                here = slice(kk * LANES, (kk + 1) * LANES)
                rest = slice((kk + 1) * LANES, n)
                inverse = inv_ref[...]
                z = dot32(b_ref[:, here], inverse)
                b_ref[:, here] = z
                if kk + 1 < blocks:
                    panel = a_ref[here, rest]
                    w = dot32(a_ref[rest, here], inverse)
                    a_ref[rest, here] = w
                    a_ref[rest, rest] = a_ref[rest, rest] - dot32(w, panel)
                    b_ref[:, rest] = b_ref[:, rest] - dot32(z, panel)

        return carry

    lax.fori_loop(0, blocks, step, 0)
    for k in range(blocks - 2, -1, -1):
        here = slice(k * LANES, (k + 1) * LANES)
        rest = slice((k + 1) * LANES, n)
        b_ref[:, here] = b_ref[:, here] - dot32(b_ref[:, rest], a_ref[rest, here])
    out_ref[...] = b_ref[...] * math.sqrt(columns) * weight_ref[...]


def solve(kernel, cross, weight, columns):
    n = kernel.shape[0]
    rows = cross.shape[0]
    return pl.pallas_call(
        functools.partial(solve_kernel, columns),
        out_shape=jax.ShapeDtypeStruct((rows, n), jnp.float32),
        in_specs=[pl.BlockSpec(memory_space=pltpu.VMEM)] * 3,
        out_specs=pl.BlockSpec(memory_space=pltpu.VMEM),
        scratch_shapes=[
            pltpu.VMEM((n, n), jnp.float32),
            pltpu.VMEM((rows, n), jnp.float32),
            pltpu.VMEM((LANES, LANES), jnp.float32),
        ],
    )(kernel, cross, weight)


def on_device(ex_grads, tgt_grads, projection, example_weight):
    ex_rows = ex_grads.shape[0]
    columns = projection.shape[1]
    param_total = lax.axis_size("param")
    param_pos = lax.axis_index("param")
    stacked = jnp.concatenate([ex_grads, tgt_grads], axis=0)
    contract_rows = (((0,), (1,)), ((), ()))
    feature_block = lax.psum_scatter(
        lax.dot_general(projection, stacked, contract_rows, preferred_element_type=jnp.float32),
        "param",
        scatter_dimension=0,
        tiled=True,
    )
    local_features = feature_block.astype(jnp.bfloat16)
    example_part = local_features[:, :ex_rows]
    contract_first = (((0,), (0,)), ((), ()))
    partial_value = lax.dot_general(
        local_features,
        lax.all_gather(example_part, "dp", axis=1, tiled=True),
        contract_first,
        preferred_element_type=jnp.float32,
    )
    examples = partial_value.shape[1]
    summed = lax.psum(partial_value, "param")
    kernel = lax.all_gather(summed[:ex_rows], "dp", axis=0, tiled=True)
    block_cols = examples // param_total
    scaled = solve(kernel, summed[ex_rows:], jnp.ones((1, examples), jnp.float32), columns)
    chosen = lax.dynamic_slice_in_dim(scaled, param_pos * block_cols, block_cols, 1)
    return chosen * example_weight[None, :]


def solution(mesh):
    placed = (P("dp", "param"), P("dp", "param"), P("param", None), P("param"))
    return jax.shard_map(
        on_device, mesh=mesh, in_specs=placed, out_specs=P("dp", "param"), check_vma=False
    )
```

```python
import functools
import math

import jax
import jax.numpy as jnp
from jax import lax
from jax.experimental import pallas as pl
from jax.experimental.pallas import tpu as pltpu
from jax.sharding import PartitionSpec as P

ridge_value = 0.5
LANES = 128
GROUP = 8


def dot32(a, b):
    return jnp.dot(a, b, preferred_element_type=jnp.float32, precision=lax.Precision.HIGHEST)


def invert_block(block):
    size = block.shape[0]
    groups = size // GROUP
    rows = [block[GROUP * i : GROUP * (i + 1), :] for i in range(groups)]
    shape = (GROUP, size)
    sub = lax.broadcasted_iota(jnp.int32, shape, 0)
    lane = lax.broadcasted_iota(jnp.int32, shape, 1)

    def lane_splat(x, c):
        return jnp.broadcast_to(x[:, c : c + 1], shape)

    def row_splat(x, j):
        return jnp.broadcast_to(x[j : j + 1, :], shape)

    for g in range(groups):
        base = GROUP * g
        panel = rows[g]
        cols = [lane_splat(panel, base + j) for j in range(GROUP)]
        in_group = (lane >= base) & (lane < base + GROUP)
        panel = jnp.where(in_group, jnp.where(sub + base == lane, 1.0, 0.0), panel)
        for j in range(GROUP):
            inv = 1.0 / row_splat(cols[j], j)
            mult = jnp.where(sub == j, 1.0 - inv, cols[j] * inv)
            for c in range(j + 1, GROUP):
                cols[c] = cols[c] - mult * row_splat(cols[c], j)
            panel = panel - mult * row_splat(panel, j)
        spread = [row_splat(panel, j) for j in range(GROUP)]
        order = list(range(g + 1, groups)) + list(range(g))
        for i in order:
            acc = jnp.where(in_group, 0.0, rows[i])
            for j in range(GROUP):
                acc = acc - lane_splat(rows[i], base + j) * spread[j]
            rows[i] = acc
        rows[g] = panel
    return jnp.concatenate(rows, axis=0)


def gather_kernel(own_ref, send_ref, out_ref, recv_ref, rs_send, rs_recv, send_sem, recv_sem):
    parts, count = out_ref.shape[0], out_ref.shape[1]
    line, pairs = count // 2, parts // 2
    d, p = lax.axis_index("dp"), lax.axis_index("param")
    a, b = d // 2, d % 2
    y, c = p // 2, p % 2

    barrier = pltpu.get_barrier_semaphore()

    def greet(dd, pp):
        pl.semaphore_signal(
            barrier, inc=1, device_id={"dp": dd, "param": pp}, device_id_type=pl.DeviceIdType.MESH
        )

    for s in range(1, parts):
        greet(d, (p + s) % parts)
    greet(2 * a + (1 - b), p)
    greet(2 * ((a + 1) % line) + b, p)
    greet(2 * ((a + line - 1) % line) + b, p)
    pl.semaphore_wait(barrier, parts + 2)

    def scatter(s):
        q = (p + s) % parts
        return pltpu.make_async_remote_copy(
            src_ref=send_ref.at[q],
            dst_ref=recv_ref.at[s - 1],
            send_sem=rs_send.at[s - 1],
            recv_sem=rs_recv.at[s - 1],
            device_id={"dp": d, "param": q},
            device_id_type=pl.DeviceIdType.MESH,
        )

    for s in range(1, parts):
        scatter(s).start()
    for s in range(1, parts):
        scatter(s).wait_recv()
    total = own_ref[p]
    for s in range(1, parts):
        total = total + recv_ref[s - 1].astype(jnp.float32)
    out_ref[p, d] = total.astype(out_ref.dtype)

    def plane(first):
        sent = []

        def copy(i, sp, sd, dd, pp):
            return pltpu.make_async_remote_copy(
                src_ref=out_ref.at[sp, sd],
                dst_ref=out_ref.at[sp, sd],
                send_sem=send_sem.at[i],
                recv_sem=recv_sem.at[sp, sd],
                device_id={"dp": dd, "param": pp},
                device_id_type=pl.DeviceIdType.MESH,
            )

        def send(cond, *args):
            i = len(sent)
            sent.append((cond, args))
            if cond is None:
                copy(i, *args).start()
            else:

                @pl.when(cond)
                def _():
                    copy(i, *args).start()

        def arrive(cond, sp, sd):
            wait = copy(0, sp, sd, d, p ^ 1).wait_recv
            if cond is None:
                wait()
            else:
                pl.when(cond)(wait)

        def to_core(cond, sp, sd):
            send(cond, sp, sd, d, 2 * y + (1 - c))

        def to_pair(cond, sp, sd):
            send(cond, sp, sd, 2 * a + (1 - b), p)

        def to_rows(cond, sp, sd):
            for t in range(1, pairs):
                send(cond, sp, sd, d, 2 * ((y + t) % pairs) + c)

        def ring(s):
            if s == 0:
                return [(None, a, 0)]
            return [(a - s >= 0, a - s, -1), (a + s < line, a + s, 1)]

        def line_block(s):
            for cond, at, sign in ring(s):
                sd = 2 * at + b
                if sign:
                    arrive(cond, p, sd)
                    onward = a - sign
                    ok = jnp.logical_and(cond, jnp.logical_and(onward >= 0, onward < line))
                    send(ok, p, sd, 2 * onward + b, p)
                else:
                    send(a + 1 < line, p, sd, 2 * (a + 1) + b, p)
                    send(a >= 1, p, sd, 2 * (a - 1) + b, p)
                to_pair(cond, p, sd)
                to_rows(cond, p, sd)
                to_core(cond, p, sd)

        def second(s):
            for cond, at, _ in ring(s):
                if first:
                    sd = 2 * at + (1 - b)
                    arrive(cond, p, sd)
                    to_rows(cond, p, sd)
                    to_core(cond, p, sd)
                else:
                    sd = 2 * at + b
                    for t in range(1, pairs):
                        sp = 2 * ((y + t) % pairs) + c
                        arrive(cond, sp, sd)
                        to_pair(cond, sp, sd)
                        to_core(cond, sp, sd)

        def third(s):
            for cond, at, _ in ring(s):
                if first:
                    for t in range(1, pairs):
                        sp = 2 * ((y + t) % pairs) + c
                        for bb in (b, 1 - b):
                            arrive(cond, sp, 2 * at + bb)
                            to_core(cond, sp, 2 * at + bb)
                else:
                    for t in range(pairs):
                        sp = 2 * ((y + t) % pairs) + c
                        arrive(cond, sp, 2 * at + (1 - b))
                        to_core(cond, sp, 2 * at + (1 - b))

        line_block(0)
        for s in range(1, line):
            line_block(s)
            second(s - 1)
        second(line - 1)
        for s in range(line):
            third(s)
        for yy in range(pairs):
            for dd in range(count):
                arrive(None, 2 * yy + (1 - c), dd)
        for i, (cond, args) in enumerate(sent):
            wait = copy(i, *args).wait_send
            if cond is None:
                wait()
            else:
                pl.when(cond)(wait)

    @pl.when(c == 0)
    def _():
        plane(True)

    @pl.when(c == 1)
    def _():
        plane(False)

    for s in range(1, parts):
        scatter(s).wait_send()


def gather_features(partial, parts, count):
    _, rows, block = partial.shape
    return pl.pallas_call(
        gather_kernel,
        out_shape=jax.ShapeDtypeStruct((parts, count, rows, block), jnp.bfloat16),
        in_specs=[pl.BlockSpec(memory_space=pltpu.VMEM)] * 2,
        out_specs=pl.BlockSpec(memory_space=pltpu.VMEM),
        scratch_shapes=[
            pltpu.VMEM((parts - 1, rows, block), jnp.bfloat16),
            pltpu.SemaphoreType.DMA((parts - 1,)),
            pltpu.SemaphoreType.DMA((parts - 1,)),
            pltpu.SemaphoreType.DMA((2 * count + 2 * parts * count,)),
            pltpu.SemaphoreType.DMA((parts, count)),
        ],
        compiler_params=pltpu.CompilerParams(collective_id=0, has_side_effects=True),
    )(partial, partial.astype(jnp.bfloat16))


def solve_kernel(columns, parts, kernel_ref, out_ref, a_ref, b_ref, inv_ref):
    n = kernel_ref.shape[0]
    rows = b_ref.shape[0]
    blocks = n // LANES
    diag = lax.broadcasted_iota(jnp.int32, (LANES, n), 0)
    col_ids = lax.broadcasted_iota(jnp.int32, (LANES, n), 1)
    for i in range(blocks):
        part = kernel_ref[i * LANES : (i + 1) * LANES, :] / columns
        a_ref[i * LANES : (i + 1) * LANES, :] = part + jnp.where(diag + i * LANES == col_ids, ridge_value, 0.0)
    first = lax.axis_index("param") * rows
    row_ids = lax.broadcasted_iota(jnp.int32, (rows, n), 0)
    b_ref[...] = jnp.where(row_ids + first == lax.broadcasted_iota(jnp.int32, (rows, n), 1), 1.0, 0.0)

    def step(k, carry):
        at = pl.multiple_of(k * LANES, LANES)
        inv_ref[...] = invert_block(a_ref[pl.ds(at, LANES), pl.ds(at, LANES)])
        for kk in range(blocks):

            @pl.when(k == kk)
            def _():
                here = slice(kk * LANES, (kk + 1) * LANES)
                rest = slice((kk + 1) * LANES, n)
                inverse = inv_ref[...]
                z = dot32(b_ref[:, here], inverse)
                b_ref[:, here] = z
                if kk + 1 < blocks:
                    panel = a_ref[here, rest]
                    w = dot32(a_ref[rest, here], inverse)
                    a_ref[rest, here] = w
                    a_ref[rest, rest] = a_ref[rest, rest] - dot32(w, panel)
                    b_ref[:, rest] = b_ref[:, rest] - dot32(z, panel)

        return carry

    lax.fori_loop(0, blocks, step, 0)
    for k in range(blocks - 2, -1, -1):
        here = slice(k * LANES, (k + 1) * LANES)
        rest = slice((k + 1) * LANES, n)
        b_ref[:, here] = b_ref[:, here] - dot32(b_ref[:, rest], a_ref[rest, here])
    out_ref[...] = b_ref[...]


def inverse_rows(kernel, columns, parts):
    n = kernel.shape[0]
    rows = n // parts
    return pl.pallas_call(
        functools.partial(solve_kernel, columns, parts),
        out_shape=jax.ShapeDtypeStruct((rows, n), jnp.float32),
        in_specs=[pl.BlockSpec(memory_space=pltpu.VMEM)],
        out_specs=pl.BlockSpec(memory_space=pltpu.VMEM),
        scratch_shapes=[
            pltpu.VMEM((n, n), jnp.float32),
            pltpu.VMEM((rows, n), jnp.float32),
            pltpu.VMEM((LANES, LANES), jnp.float32),
        ],
        cost_estimate=pl.CostEstimate(flops=40 * n**3, bytes_accessed=8 * n * n, transcendentals=0),
    )(kernel)


def on_device(ex_grads, tgt_grads, projection, example_weight):
    ex_rows = ex_grads.shape[0]
    columns = projection.shape[1]
    parts = lax.axis_size("param")
    count = lax.axis_size("dp")
    examples = ex_rows * count
    partial = jnp.dot(ex_grads, projection, preferred_element_type=jnp.float32)
    partial = partial.reshape(ex_rows, parts, columns // parts).transpose(1, 0, 2)
    features = gather_features(partial, parts, count).reshape(parts, examples, columns // parts)
    kernel = sum(
        lax.dot_general(
            features[q], features[q], (((1,), (1,)), ((), ())), preferred_element_type=jnp.float32
        )
        for q in range(parts)
    )
    spread = features.transpose(1, 0, 2).reshape(examples, columns)
    mixed = lax.dot_general(
        projection, spread, (((1,), (1,)), ((), ())), preferred_element_type=jnp.float32
    )
    head = lax.reduce_precision(mixed, 8, 7)
    tail = (mixed - head).astype(jnp.bfloat16)
    cross = jnp.dot(tgt_grads, head.astype(jnp.bfloat16), preferred_element_type=jnp.float32)
    cross = cross + jnp.dot(tgt_grads, tail, preferred_element_type=jnp.float32)
    cross = lax.psum(cross, "param") / columns
    chosen = inverse_rows(kernel, columns, parts)
    scores = lax.dot_general(
        cross,
        chosen,
        (((1,), (1,)), ((), ())),
        precision=lax.Precision.HIGHEST,
        preferred_element_type=jnp.float32,
    )
    return scores * math.sqrt(columns) * example_weight[None, :]


def solution(mesh):
    placed = (P("dp", "param"), P("dp", "param"), P("param", None), P("param"))
    return jax.shard_map(
        on_device, mesh=mesh, in_specs=placed, out_specs=P("dp", "param"), check_vma=False
    )
```

```python
import functools
import math

import jax
import jax.numpy as jnp
from jax import lax
from jax.experimental import pallas as pl
from jax.experimental.pallas import tpu as pltpu
from jax.sharding import PartitionSpec as P

ridge_value = 0.5
LANES = 128
GROUP = 8


def dot32(a, b):
    return jnp.dot(a, b, preferred_element_type=jnp.float32, precision=lax.Precision.HIGHEST)


def invert_block(block):
    size = block.shape[0]
    groups = size // GROUP
    rows = [block[GROUP * i : GROUP * (i + 1), :] for i in range(groups)]
    shape = (GROUP, size)
    sub = lax.broadcasted_iota(jnp.int32, shape, 0)
    lane = lax.broadcasted_iota(jnp.int32, shape, 1)

    def lane_splat(x, c):
        return jnp.broadcast_to(x[:, c : c + 1], shape)

    def row_splat(x, j):
        return jnp.broadcast_to(x[j : j + 1, :], shape)

    for g in range(groups):
        base = GROUP * g
        panel = rows[g]
        cols = [lane_splat(panel, base + j) for j in range(GROUP)]
        in_group = (lane >= base) & (lane < base + GROUP)
        panel = jnp.where(in_group, jnp.where(sub + base == lane, 1.0, 0.0), panel)
        for j in range(GROUP):
            inv = 1.0 / row_splat(cols[j], j)
            mult = jnp.where(sub == j, 1.0 - inv, cols[j] * inv)
            for c in range(j + 1, GROUP):
                cols[c] = cols[c] - mult * row_splat(cols[c], j)
            panel = panel - mult * row_splat(panel, j)
        spread = [row_splat(panel, j) for j in range(GROUP)]
        order = list(range(g + 1, groups)) + list(range(g))
        for i in order:
            acc = jnp.where(in_group, 0.0, rows[i])
            for j in range(GROUP):
                acc = acc - lane_splat(rows[i], base + j) * spread[j]
            rows[i] = acc
        rows[g] = panel
    return jnp.concatenate(rows, axis=0)


def gather_kernel(own_ref, send_ref, out_ref, recv_ref, rs_send, rs_recv, send_sem, recv_sem):
    parts, count = lax.axis_size("param"), out_ref.shape[0]
    block = out_ref.shape[2] // parts
    line, pairs = count // 2, parts // 2
    d, p = lax.axis_index("dp"), lax.axis_index("param")
    a, b = d // 2, d % 2
    y, c = p // 2, p % 2

    def part(sp):
        return pl.ds(pl.multiple_of(sp * block, LANES), block)

    barrier = pltpu.get_barrier_semaphore()

    def greet(dd, pp):
        pl.semaphore_signal(
            barrier, inc=1, device_id={"dp": dd, "param": pp}, device_id_type=pl.DeviceIdType.MESH
        )

    for s in range(1, parts):
        greet(d, (p + s) % parts)
    greet(2 * a + (1 - b), p)
    greet(2 * ((a + 1) % line) + b, p)
    greet(2 * ((a + line - 1) % line) + b, p)
    pl.semaphore_wait(barrier, parts + 2)

    def scatter(s):
        q = (p + s) % parts
        return pltpu.make_async_remote_copy(
            src_ref=send_ref.at[:, part(q)],
            dst_ref=recv_ref.at[s - 1],
            send_sem=rs_send.at[s - 1],
            recv_sem=rs_recv.at[s - 1],
            device_id={"dp": d, "param": q},
            device_id_type=pl.DeviceIdType.MESH,
        )

    for s in range(1, parts):
        scatter(s).start()
    for s in range(1, parts):
        scatter(s).wait_recv()
    total = own_ref[:, part(p)]
    for s in range(1, parts):
        total = total + recv_ref[s - 1].astype(jnp.float32)
    out_ref[d, :, part(p)] = total.astype(out_ref.dtype)

    def plane(first):
        sent = []

        def copy(i, sp, sd, dd, pp):
            return pltpu.make_async_remote_copy(
                src_ref=out_ref.at[sd, :, part(sp)],
                dst_ref=out_ref.at[sd, :, part(sp)],
                send_sem=send_sem.at[i],
                recv_sem=recv_sem.at[sp, sd],
                device_id={"dp": dd, "param": pp},
                device_id_type=pl.DeviceIdType.MESH,
            )

        def send(cond, *args):
            i = len(sent)
            sent.append((cond, args))
            if cond is None:
                copy(i, *args).start()
            else:

                @pl.when(cond)
                def _():
                    copy(i, *args).start()

        def arrive(cond, sp, sd):
            wait = copy(0, sp, sd, d, p ^ 1).wait_recv
            if cond is None:
                wait()
            else:
                pl.when(cond)(wait)

        def to_core(cond, sp, sd):
            send(cond, sp, sd, d, 2 * y + (1 - c))

        def to_pair(cond, sp, sd):
            send(cond, sp, sd, 2 * a + (1 - b), p)

        def to_rows(cond, sp, sd):
            for t in range(1, pairs):
                send(cond, sp, sd, d, 2 * ((y + t) % pairs) + c)

        def ring(s):
            if s == 0:
                return [(None, a, 0)]
            return [(a - s >= 0, a - s, -1), (a + s < line, a + s, 1)]

        def line_block(s):
            for cond, at, sign in ring(s):
                sd = 2 * at + b
                if sign:
                    arrive(cond, p, sd)
                    onward = a - sign
                    ok = jnp.logical_and(cond, jnp.logical_and(onward >= 0, onward < line))
                    send(ok, p, sd, 2 * onward + b, p)
                else:
                    send(a + 1 < line, p, sd, 2 * (a + 1) + b, p)
                    send(a >= 1, p, sd, 2 * (a - 1) + b, p)
                to_pair(cond, p, sd)
                to_rows(cond, p, sd)
                to_core(cond, p, sd)

        def second(s):
            for cond, at, _ in ring(s):
                if first:
                    sd = 2 * at + (1 - b)
                    arrive(cond, p, sd)
                    to_rows(cond, p, sd)
                    to_core(cond, p, sd)
                else:
                    sd = 2 * at + b
                    for t in range(1, pairs):
                        sp = 2 * ((y + t) % pairs) + c
                        arrive(cond, sp, sd)
                        to_pair(cond, sp, sd)
                        to_core(cond, sp, sd)

        def third(s):
            for cond, at, _ in ring(s):
                if first:
                    for t in range(1, pairs):
                        sp = 2 * ((y + t) % pairs) + c
                        for bb in (b, 1 - b):
                            arrive(cond, sp, 2 * at + bb)
                            to_core(cond, sp, 2 * at + bb)
                else:
                    for t in range(pairs):
                        sp = 2 * ((y + t) % pairs) + c
                        arrive(cond, sp, 2 * at + (1 - b))
                        to_core(cond, sp, 2 * at + (1 - b))

        line_block(0)
        for s in range(1, line):
            line_block(s)
            second(s - 1)
        second(line - 1)
        for s in range(line):
            third(s)
        for yy in range(pairs):
            for dd in range(count):
                arrive(None, 2 * yy + (1 - c), dd)
        for i, (cond, args) in enumerate(sent):
            wait = copy(i, *args).wait_send
            if cond is None:
                wait()
            else:
                pl.when(cond)(wait)

    @pl.when(c == 0)
    def _():
        plane(True)

    @pl.when(c == 1)
    def _():
        plane(False)

    for s in range(1, parts):
        scatter(s).wait_send()


def gather_features(partial, parts, count):
    rows, columns = partial.shape
    block = columns // parts
    return pl.pallas_call(
        gather_kernel,
        out_shape=jax.ShapeDtypeStruct((count, rows, columns), jnp.bfloat16),
        in_specs=[pl.BlockSpec(memory_space=pltpu.VMEM)] * 2,
        out_specs=pl.BlockSpec(memory_space=pltpu.VMEM),
        scratch_shapes=[
            pltpu.VMEM((parts - 1, rows, block), jnp.bfloat16),
            pltpu.SemaphoreType.DMA((parts - 1,)),
            pltpu.SemaphoreType.DMA((parts - 1,)),
            pltpu.SemaphoreType.DMA((2 * count + 2 * parts * count,)),
            pltpu.SemaphoreType.DMA((parts, count)),
        ],
        compiler_params=pltpu.CompilerParams(collective_id=0, has_side_effects=True),
    )(partial, partial.astype(jnp.bfloat16))


def solve_kernel(columns, parts, kernel_ref, out_ref, a_ref, b_ref, inv_ref):
    n = kernel_ref.shape[0]
    rows = b_ref.shape[0]
    blocks = n // LANES
    diag = lax.broadcasted_iota(jnp.int32, (LANES, n), 0)
    col_ids = lax.broadcasted_iota(jnp.int32, (LANES, n), 1)
    for i in range(blocks):
        part = kernel_ref[i * LANES : (i + 1) * LANES, :] / columns
        a_ref[i * LANES : (i + 1) * LANES, :] = part + jnp.where(diag + i * LANES == col_ids, ridge_value, 0.0)
    first = lax.axis_index("param") * rows
    row_ids = lax.broadcasted_iota(jnp.int32, (rows, n), 0)
    b_ref[...] = jnp.where(row_ids + first == lax.broadcasted_iota(jnp.int32, (rows, n), 1), 1.0, 0.0)

    def step(k, carry):
        at = pl.multiple_of(k * LANES, LANES)
        inv_ref[...] = invert_block(a_ref[pl.ds(at, LANES), pl.ds(at, LANES)])
        for kk in range(blocks):

            @pl.when(k == kk)
            def _():
                here = slice(kk * LANES, (kk + 1) * LANES)
                rest = slice((kk + 1) * LANES, n)
                inverse = inv_ref[...]
                z = dot32(b_ref[:, here], inverse)
                b_ref[:, here] = z
                if kk + 1 < blocks:
                    panel = a_ref[here, rest]
                    w = dot32(a_ref[rest, here], inverse)
                    a_ref[rest, here] = w
                    a_ref[rest, rest] = a_ref[rest, rest] - dot32(w, panel)
                    b_ref[:, rest] = b_ref[:, rest] - dot32(z, panel)

        return carry

    lax.fori_loop(0, blocks, step, 0)
    for k in range(blocks - 2, -1, -1):
        here = slice(k * LANES, (k + 1) * LANES)
        rest = slice((k + 1) * LANES, n)
        b_ref[:, here] = b_ref[:, here] - dot32(b_ref[:, rest], a_ref[rest, here])
    out_ref[...] = b_ref[...]


def inverse_rows(kernel, columns, parts):
    n = kernel.shape[0]
    rows = n // parts
    return pl.pallas_call(
        functools.partial(solve_kernel, columns, parts),
        out_shape=jax.ShapeDtypeStruct((rows, n), jnp.float32),
        in_specs=[pl.BlockSpec(memory_space=pltpu.VMEM)],
        out_specs=pl.BlockSpec(memory_space=pltpu.VMEM),
        scratch_shapes=[
            pltpu.VMEM((n, n), jnp.float32),
            pltpu.VMEM((rows, n), jnp.float32),
            pltpu.VMEM((LANES, LANES), jnp.float32),
        ],
        cost_estimate=pl.CostEstimate(flops=40 * n**3, bytes_accessed=8 * n * n, transcendentals=0),
    )(kernel)


def on_device(ex_grads, tgt_grads, projection, example_weight):
    ex_rows = ex_grads.shape[0]
    columns = projection.shape[1]
    parts = lax.axis_size("param")
    count = lax.axis_size("dp")
    examples = ex_rows * count
    partial = jnp.dot(ex_grads, projection, preferred_element_type=jnp.float32)
    features = gather_features(partial, parts, count).reshape(examples, columns)
    contract_last = (((1,), (1,)), ((), ()))
    kernel = lax.dot_general(features, features, contract_last, preferred_element_type=jnp.float32)
    mixed = lax.dot_general(projection, features, contract_last, preferred_element_type=jnp.float32)
    head = lax.reduce_precision(mixed, 8, 7)
    tail = (mixed - head).astype(jnp.bfloat16)
    cross = jnp.dot(tgt_grads, head.astype(jnp.bfloat16), preferred_element_type=jnp.float32)
    cross = cross + jnp.dot(tgt_grads, tail, preferred_element_type=jnp.float32)
    cross = lax.psum(cross, "param") / columns
    chosen = inverse_rows(kernel, columns, parts)
    scores = lax.dot_general(
        cross,
        chosen,
        (((1,), (1,)), ((), ())),
        precision=lax.Precision.HIGHEST,
        preferred_element_type=jnp.float32,
    )
    return scores * math.sqrt(columns) * example_weight[None, :]


def solution(mesh):
    placed = (P("dp", "param"), P("dp", "param"), P("param", None), P("param"))
    return jax.shard_map(
        on_device, mesh=mesh, in_specs=placed, out_specs=P("dp", "param"), check_vma=False
    )
```
